32 devices in a mesh: dev: 8 (over y, x, core), ka: 4 (over z).
Axes of the slice: x: 2, y: 2, z: 4, core: 2. Of those that a mesh axis runs over, the one named last changes fastest.
Arguments:
- tile_data: float32 [2048, 128, 128], P(('dev', 'ka')), may hold values from -0.25 to 0.25
- tile_row: int32 [32, 64], P(('dev', 'ka')), may hold values from 0 to 31
- tile_col: int32 [32, 64], P(('dev', 'ka')), may hold values from 0 to 63
- tile_count: int32 [32], P(('dev', 'ka')), may hold values from 10 to 64, as said below
- touched: int32 [32, 64], P(('dev', 'ka')), may hold values from 0 to 127, as said below
- owner_map: int32 [128], replicated, may hold values from 0 to 127, as said below
- observed: float32 [1024, 128, 64], P(('dev', 'ka')), may hold values from -6 to 6
- start_x: float32 [2048, 128, 64], P(('dev', 'ka')), may hold values from -6 to 6
- start_u: float32 [2048, 128, 64], P(('dev', 'ka')), may hold values from -4 to 4
Outputs:
- final_x: float32 [2048, 128, 64], P(('dev', 'ka'))
- final_u: float32 [2048, 128, 64], P(('dev', 'ka'))
- z_keeper_agreed: float32 [128, 128, 64], P(('dev', 'ka'))
- primal_gap: float32 [64], replicated
The draws below stay inside these ranges and needn't reach their ends.
Inputs may be any that keep to these rules, and one draw needn't show every extreme that they name: Shard s uses its first tile_count[s] slots; each count is at least 10 and at most 64, and some shard has exactly 64. `touched`: A shard's 64 entries are distinct column blocks. The owner of block j is shard owner_map[j] // 4; a shard touches at most 2 blocks of one owner, and every shard touches exactly 2 blocks of some owner. `owner_map`: A permutation of 0 to 127.
All inputs are finite; a program needn't handle non-finite values.
Results may differ from the reference program's by a relative error of at most 0.0003.
Values sent between devices are 32-bit elements.
A program may use at most 128 MiB of HBM per device.

```python
import math
import jax
import jax.numpy as jnp
import numpy as np
from jax import lax

BLK = 128
TARGETS = 64
TILE_DEV = 64
ROWB_DEV = 32
LOCAL_COLS = 64
COL_DEV = 4
ITERS = 2
CG_STEPS = 4
PIECE_TOTAL = 32
OWNER_LIMIT = 2
COLB = 128
TILES = 2048
ROWBLOCKS = 1024
SLOTS = 2048


def column_plan(key):
    ordering = jax.random.permutation(jax.random.fold_in(key, 11), COLB).astype(jnp.int32)
    inverse = jnp.zeros((COLB,), jnp.int32).at[ordering].set(jnp.arange(COLB, dtype=jnp.int32))
    keeper_demand = jax.random.randint(jax.random.fold_in(key, 12), (PIECE_TOTAL,), 0, 8, dtype=jnp.int32)
    block_heat = jax.random.randint(jax.random.fold_in(key, 13), (PIECE_TOTAL, COL_DEV), 0, 8, dtype=jnp.int32)
    local_noise = jax.random.randint(jax.random.fold_in(key, 14), (PIECE_TOTAL, PIECE_TOTAL, COL_DEV), 0, 1024, dtype=jnp.int32)
    local_score = local_noise * (1 + block_heat * block_heat)[None, :, :] * COL_DEV + jnp.arange(COL_DEV, dtype=jnp.int32)
    local_pick = lax.top_k(local_score, OWNER_LIMIT)[1].astype(jnp.int32)
    couple_jitter = jax.random.randint(jax.random.fold_in(key, 15), (PIECE_TOTAL, PIECE_TOTAL, OWNER_LIMIT), 0, 1024, dtype=jnp.int32)
    preferred_keeper = jax.random.randint(jax.random.fold_in(key, 16), (PIECE_TOTAL,), 0, PIECE_TOTAL, dtype=jnp.int32)
    preference_reward = (jnp.arange(PIECE_TOTAL, dtype=jnp.int32)[None, :] == preferred_keeper[:, None]).astype(jnp.int32) * (1 << 28)
    couple_position = jnp.arange(PIECE_TOTAL * OWNER_LIMIT, dtype=jnp.int32).reshape(PIECE_TOTAL, OWNER_LIMIT)
    couple_rating = couple_jitter * (1 + keeper_demand * keeper_demand)[None, :, None] * (PIECE_TOTAL * OWNER_LIMIT) + couple_position[None, :, :] + preference_reward[:, :, None]
    chosen = lax.top_k(couple_rating.reshape(PIECE_TOTAL, PIECE_TOTAL * OWNER_LIMIT), LOCAL_COLS)[1].astype(jnp.int32)
    owners = chosen // OWNER_LIMIT
    local_ids = jnp.take_along_axis(local_pick.reshape(PIECE_TOTAL, PIECE_TOTAL * OWNER_LIMIT), chosen, axis=1)
    touched_ids = inverse[owners * COL_DEV + local_ids]
    return (ordering, touched_ids.astype(jnp.int32))


def draw_touched(key, part):
    return column_plan(key)[1]


def draw_owner_map(key, part):
    return column_plan(key)[0]


def draw_tile_count(key, part):
    levels = jax.random.randint(jax.random.fold_in(key, 3), (PIECE_TOTAL,), 0, 6, dtype=jnp.int32)
    counts = TILE_DEV // (1 + levels)
    busiest = jax.random.randint(jax.random.fold_in(key, 4), (), 0, PIECE_TOTAL, dtype=jnp.int32)
    return jnp.where(jnp.arange(PIECE_TOTAL, dtype=jnp.int32) == busiest, TILE_DEV, counts).astype(jnp.int32)


def touch_ends(drawn, key, least, largest):
    longest = drawn.shape.index(max(drawn.shape))
    spots = []
    for shift in (0, 1):
        where = [jax.random.randint(jax.random.fold_in(key, axis), (), 0, length) for axis, length in enumerate(drawn.shape)]
        where[longest] = (where[longest] + shift) % drawn.shape[longest]
        spots.append(tuple(where))
    return drawn.at[spots[0]].set(least).at[spots[1]].set(largest)


def block_levels(key, extent, pieces, low, top_value):
    factor_of = 1.0
    for position, shards_of in pieces:
        steps = jax.random.uniform(jax.random.fold_in(jax.random.fold_in(key, 6), position), (shards_of,), jnp.float32, low / len(pieces), top_value / len(pieces))
        factor_of = factor_of * jnp.repeat(jnp.exp(steps), extent[position] // shards_of).reshape((-1,) + (1,) * (len(extent) - 1 - position))
    return factor_of


def cumulative_ranks(number_of, lean):
    loads = [(1 << 20) // math.isqrt(standing ** lean) + 1 for standing in range(1, number_of + 1)]
    width = 1 + sum(loads) // (1 << 30)
    return np.cumsum(np.array([max(1, weight // width) for weight in loads]))


def ranked(own_key, shape, count, slope):
    table = cumulative_ranks(count, slope)
    lot = jax.random.randint(jax.random.fold_in(own_key, 1), shape, 0, int(table[count - 1]))
    rank = jnp.searchsorted(jnp.asarray(table, jnp.int32), lot, side="right")
    return jax.random.permutation(jax.random.fold_in(own_key, 2), count)[rank].astype(jnp.int32)


def normal_values(own_key, shape, scale, most, split=(), kind=jnp.bfloat16):
    level = block_levels(own_key, shape, split, -0.22, 0.18) if split else 1.0
    drawn = jax.random.normal(own_key, shape, jnp.float32) * scale * level
    return jnp.minimum(jnp.maximum(drawn, -most), most).astype(kind)


def setup_inputs(seed: int = 0) -> dict:
    splits = jax.random.split(jax.random.key(seed), 10)
    tile_data = normal_values(splits[0], (TILES, BLK, BLK), (4 * BLK) ** -0.5, 0.25, ((0, 32),), jnp.float32)
    tile_row = touch_ends(jax.random.randint(splits[1], (PIECE_TOTAL, TILE_DEV), 0, ROWB_DEV), jax.random.fold_in(splits[1], 1), 0, ROWB_DEV - 1).astype(jnp.int32)
    tile_col = touch_ends(ranked(splits[2], (PIECE_TOTAL, TILE_DEV), LOCAL_COLS, 2), jax.random.fold_in(splits[2], 3), 0, LOCAL_COLS - 1).astype(jnp.int32)
    tile_count = draw_tile_count(jax.random.fold_in(splits[9], 71), 0)
    touched = draw_touched(jax.random.fold_in(splits[9], 71), 0)
    owner_map = draw_owner_map(jax.random.fold_in(splits[9], 71), 0)
    observed = normal_values(splits[6], (ROWBLOCKS, BLK, TARGETS), 1.0, 6.0, ((0, 32),), jnp.float32)
    start_x = normal_values(splits[7], (SLOTS, BLK, TARGETS), 1.0, 6.0, ((0, 32),), jnp.float32)
    start_u = normal_values(splits[8], (SLOTS, BLK, TARGETS), 0.5, 4.0, ((0, 32),), jnp.float32)
    return dict(tile_data=tile_data, tile_row=tile_row, tile_col=tile_col, tile_count=tile_count, touched=touched, owner_map=owner_map, observed=observed, start_x=start_x, start_u=start_u)


EXACTNESS = lax.Precision.HIGHEST
PENALTY = 1.0
COUPLING = 1.0

def shrink(amount, cutoff):
    return amount - jnp.clip(amount, -cutoff, cutoff)

def forward(tile_set, row_ids, col_ids, in_use, vector):
    product = jnp.einsum('tij,tjr->tir', tile_set, vector[col_ids], precision=EXACTNESS) * in_use[:, None, None]
    return jax.ops.segment_sum(product, row_ids, ROWB_DEV)

def backward(tile_set, row_ids, col_ids, in_use, vector):
    product = jnp.einsum('tji,tjr->tir', tile_set, vector[row_ids], precision=EXACTNESS) * in_use[:, None, None]
    return jax.ops.segment_sum(product, col_ids, LOCAL_COLS)

def pull_one(packed):
    tile_set, row_ids, col_ids, in_use, observed_set = packed
    return backward(tile_set, row_ids, col_ids, in_use, observed_set)

def conjugate(packed):
    tile_set, row_ids, col_ids, in_use, rhs_side, begin = packed

    def operate(vector):
        image_rows = forward(tile_set, row_ids, col_ids, in_use, vector)
        return backward(tile_set, row_ids, col_ids, in_use, image_rows) + COUPLING * vector
    iterate = begin
    residual = rhs_side - operate(begin)
    direction = residual
    norm_now = lax.optimization_barrier(jnp.sum(residual * residual, axis=(0, 1)))
    for cg_step in range(CG_STEPS):
        mapped = operate(direction)
        step_size = norm_now / lax.optimization_barrier(jnp.sum(direction * mapped, axis=(0, 1)))
        iterate = iterate + step_size * direction
        residual = residual - step_size * mapped
        norm_next = lax.optimization_barrier(jnp.sum(residual * residual, axis=(0, 1)))
        direction = residual + norm_next / norm_now * direction
        norm_now = norm_next
    return iterate

def reference(tile_data, tile_row, tile_col, tile_count, touched, owner_map, observed, start_x, start_u):
    tile_sets = tile_data.reshape(PIECE_TOTAL, TILE_DEV, BLK, BLK)
    observed_sets = observed.reshape(PIECE_TOTAL, ROWB_DEV, BLK, TARGETS)
    current_x = start_x.reshape(PIECE_TOTAL, LOCAL_COLS, BLK, TARGETS)
    current_u = start_u.reshape(PIECE_TOTAL, LOCAL_COLS, BLK, TARGETS)
    in_use = (jnp.arange(TILE_DEV, dtype=jnp.int32)[None, :] < tile_count[:, None]).astype(jnp.float32)
    pulled = lax.map(pull_one, (tile_sets, tile_row, tile_col, in_use, observed_sets))
    flat_ids = touched.reshape(-1)
    counts = jax.ops.segment_sum(jnp.ones(flat_ids.shape, jnp.float32), flat_ids, COLB)
    share = jnp.maximum(counts, 1.0)[:, None, None]
    consensus = jnp.zeros((COLB, BLK, TARGETS), jnp.float32)
    difference = jnp.zeros_like(current_x)
    for outer_step in range(ITERS):
        merged = (current_x + current_u).reshape(SLOTS, BLK, TARGETS)
        summed = jax.ops.segment_sum(merged, flat_ids, COLB)
        consensus = shrink(summed / share, PENALTY / (COUPLING * share))
        z_local = consensus[touched]
        difference = current_x - z_local
        current_u = current_u + difference
        rhs_side = pulled + COUPLING * (z_local - current_u)
        current_x = lax.map(conjugate, (tile_sets, tile_row, tile_col, in_use, rhs_side, current_x))
    primal_gap = jnp.sqrt(lax.optimization_barrier(jnp.sum(difference * difference, axis=(0, 1, 2))) / (PIECE_TOTAL * LOCAL_COLS * BLK))
    z_keeper_agreed = jnp.zeros_like(consensus).at[owner_map].set(consensus)
    return (current_x.reshape(SLOTS, BLK, TARGETS), current_u.reshape(SLOTS, BLK, TARGETS), z_keeper_agreed, primal_gap)
```

```python
import functools
import math

import jax
import jax.numpy as jnp
from jax import lax
from jax.experimental import pallas as pl
from jax.experimental.pallas import tpu as pltpu
from jax.sharding import PartitionSpec as P

ITERS = 2
CG_STEPS = 4
PENALTY = 1.0
COUPLING = 1.0
AXES = ("dev", "ka")
MESH = pl.DeviceIdType.MESH
MIB = 1 << 20


def vmem():
    return pl.BlockSpec(memory_space=pltpu.VMEM)


def smem():
    return pl.BlockSpec(memory_space=pltpu.SMEM)


def split(value):
    high = value.astype(jnp.bfloat16)
    low = (value - high.astype(jnp.float32)).astype(jnp.bfloat16)
    return jnp.concatenate([high, low], axis=0)


def tile_pass(tiles_ref, from_ids, to_ids, in_count, source_ref, target_ref):
    group = math.gcd(16, tiles_ref.shape[0])
    half = source_ref.shape[1] // 2

    def add_group(number, carry):
        for inner in range(group):
            t = number * group + inner
            lhs = source_ref[from_ids[0, t]]
            out = jnp.dot(
                jnp.concatenate([lhs, lhs], axis=1),
                tiles_ref[t],
                preferred_element_type=jnp.float32,
            )
            landing = to_ids[0, t]
            target_ref[landing] = target_ref[landing] + (out[:half] + out[half:])
        return carry

    lax.fori_loop(0, (in_count + group - 1) // group, add_group, 0)


def fill_zero(ref):
    def one(i, carry):
        ref[i] = jnp.zeros(ref.shape[1:], ref.dtype)
        return carry

    lax.fori_loop(0, ref.shape[0], one, 0, unroll=4)


def lanes(total):
    return jnp.sum(total, axis=1, keepdims=True)


def prepare_kernel(
    rows, cols, count, mailbox, tile_ref, obs_ref, x_ref, u_ref,
    fwd_ref, bwd_ref, base_ref, box_ref, xb_ref, w_ref, wb_ref,
):
    in_count = count[0]
    slots = tile_ref.shape[0]
    local_cols, targets, blk = x_ref.shape

    if box_ref.shape[0] != local_cols:
        fill_zero(box_ref)

    def convert(t, carry):
        tile = jnp.where(t < in_count, tile_ref[t], 0.0)
        bwd_ref[t] = split(tile)
        fwd_ref[t] = split(tile.T)
        return carry

    lax.fori_loop(0, slots, convert, 0, unroll=4)

    def begin(c, carry):
        x = x_ref[c]
        box_ref[mailbox[0, c]] = x + u_ref[c]
        xb_ref[c] = split(x)
        base_ref[c] = -x * COUPLING
        return carry

    lax.fori_loop(0, local_cols, begin, 0, unroll=4)
    fill_zero(w_ref)
    tile_pass(fwd_ref, cols, rows, in_count, xb_ref, w_ref)

    def against(r, carry):
        wb_ref[r] = split(obs_ref[r] - w_ref[r])
        return carry

    lax.fori_loop(0, w_ref.shape[0], against, 0, unroll=4)
    tile_pass(bwd_ref, rows, cols, in_count, wb_ref, base_ref)


def solve_kernel(
    last, rows, cols, count, mailbox, fwd_ref, bwd_ref, base_ref, x_ref, u_ref, zbox_ref,
    newx_ref, newu_ref, *rest,
):
    if last:
        gap_ref, r_ref, p_ref, q_ref, pb_ref, w_ref, wb_ref = rest
    else:
        box_ref, r_ref, p_ref, q_ref, pb_ref, w_ref, wb_ref = rest
    in_count = count[0]
    local_cols, targets, blk = x_ref.shape
    row_blocks = w_ref.shape[0]
    zero = jnp.zeros((targets, blk), jnp.float32)

    def begin(c, carry):
        rr, gap = carry
        z = zbox_ref[mailbox[0, c]]
        d = x_ref[c] - z
        u = u_ref[c] + d
        newu_ref[c] = u
        newx_ref[c] = x_ref[c]
        r = base_ref[c] + COUPLING * (z - u)
        r_ref[c] = r
        p_ref[c] = r
        q_ref[c] = COUPLING * r
        pb_ref[c] = split(r)
        return rr + r * r, gap + d * d

    rr, gap = lax.fori_loop(0, local_cols, begin, (zero, zero), unroll=2)
    if last:
        gap_ref[...] = gap
    rr = lanes(rr)
    pp = rr
    for step in range(CG_STEPS):
        final = last and step == CG_STEPS - 1
        fill_zero(w_ref)
        tile_pass(fwd_ref, cols, rows, in_count, pb_ref, w_ref)

        def image(i, ww):
            w = w_ref[i]
            if not final:
                wb_ref[i] = split(w)
            return ww + w * w

        ww = lanes(lax.fori_loop(0, row_blocks, image, zero, unroll=4))
        size = rr / (ww + COUPLING * pp)
        if final:

            def finish(c, carry):
                newx_ref[c] = newx_ref[c] + size * p_ref[c]
                return carry

            lax.fori_loop(0, local_cols, finish, 0, unroll=4)
            break
        tile_pass(bwd_ref, rows, cols, in_count, wb_ref, q_ref)

        def reduce(c, total):
            r = r_ref[c] - size * q_ref[c]
            r_ref[c] = r
            return total + r * r

        if step == CG_STEPS - 1:

            def close(c, carry):
                x = newx_ref[c] + size * p_ref[c]
                newx_ref[c] = x
                r = r_ref[c] - size * q_ref[c]
                slot = mailbox[0, c]
                u = newu_ref[c]
                box_ref[slot] = x + u
                base_ref_out[c] = r - COUPLING * (zbox_ref[slot] - u)
                return carry

            base_ref_out = r_ref
            if box_ref.shape[0] != local_cols:
                fill_zero(box_ref)
            lax.fori_loop(0, local_cols, close, 0, unroll=2)
            break
        norm = lanes(lax.fori_loop(0, local_cols, reduce, zero, unroll=4))
        turn = norm / rr

        def direct(c, total):
            old = p_ref[c]
            newx_ref[c] = newx_ref[c] + size * old
            p = r_ref[c] + turn * old
            p_ref[c] = p
            q_ref[c] = COUPLING * p
            pb_ref[c] = split(p)
            return total + p * p

        pp = lanes(lax.fori_loop(0, local_cols, direct, zero, unroll=2))
        rr = norm


def agree_kernel(
    first, n, capacity, col_dev, box_ref, tag_ref, zbox_ref, zown_ref, *rest
):
    if first:
        got_ref, inbox, ans, send, recv, send_back, recv_back, tag_send, tag_recv = rest
    else:
        inbox, ans, send, recv, send_back, recv_back = rest
        got_ref = tag_ref
    ka = lax.axis_size(AXES[1])
    me = lax.axis_index(AXES[0]) * ka + lax.axis_index(AXES[1])

    def place(device):
        return (device // ka, lax.rem(device, ka))

    def after(i):
        return lax.rem(me + i, n)

    def before(i):
        return lax.rem(me + n - i, n)

    def tags_to(i):
        return pltpu.make_async_remote_copy(
            tag_ref.at[after(i)], got_ref.at[me], tag_send.at[i], tag_recv.at[i],
            device_id=place(after(i)), device_id_type=MESH,
        )

    def tags_from(i):
        return pltpu.make_async_remote_copy(
            tag_ref.at[before(i)], got_ref.at[before(i)], tag_send.at[i], tag_recv.at[i],
            device_id=place(before(i)), device_id_type=MESH,
        )

    def part(device):
        return pl.ds(device * capacity, capacity)

    def copy(i, source, target, send_sem, recv_sem):
        return pltpu.make_async_remote_copy(
            source.at[part(after(i))], target.at[part(me)], send_sem.at[i], recv_sem.at[i],
            device_id=place(after(i)), device_id_type=MESH,
        )

    def arrival(i, source, target, send_sem, recv_sem):
        return pltpu.make_async_remote_copy(
            source.at[part(before(i))], target.at[part(before(i))], send_sem.at[i],
            recv_sem.at[i], device_id=place(before(i)), device_id_type=MESH,
        )

    def start(i, carry):
        if first:
            tags_to(i).start()
        copy(i, box_ref, inbox, send, recv).start()
        return carry

    lax.fori_loop(1, n, start, 0)
    if first:
        got_ref[me] = tag_ref[me]

    def take(source_ref, device, sums):
        counts = []
        for j in range(capacity):
            value = source_ref[device * capacity + j]
            tag = got_ref[device, pl.ds(j, 1)]
            for k in range(col_dev):
                zown_ref[k] = zown_ref[k] + jnp.where(tag == k, value, 0.0)
                counts.append((k, jnp.where(tag == k, 1.0, 0.0)))
        sums = list(sums)
        for k, hit in counts:
            sums[k] = sums[k] + hit
        return tuple(sums)

    for k in range(col_dev):
        zown_ref[k] = jnp.zeros(zown_ref.shape[1:], jnp.float32)
    none = jnp.zeros((1, zown_ref.shape[2]), jnp.float32)
    shares = take(box_ref, me, (none,) * col_dev)

    def collect(i, shares):
        if first:
            tags_from(i).wait_recv()
        arrival(i, box_ref, inbox, send, recv).wait_recv()
        return take(inbox, before(i), shares)

    shares = lax.fori_loop(1, n, collect, shares)
    for k in range(col_dev):
        share = jnp.maximum(shares[k], 1.0)
        amount = zown_ref[k] / share
        cutoff = PENALTY / (COUPLING * share)
        zown_ref[k] = amount - jnp.clip(amount, -cutoff, cutoff)

    def answer(device, target_ref):
        for j in range(capacity):
            tag = got_ref[device, pl.ds(j, 1)]
            value = jnp.zeros(zown_ref.shape[1:], jnp.float32)
            for k in range(col_dev):
                value = value + jnp.where(tag == k, zown_ref[k], 0.0)
            target_ref[device * capacity + j] = value

    def reply(i, carry):
        answer(after(i), ans)
        copy(i, ans, zbox_ref, send_back, recv_back).start()
        return carry

    lax.fori_loop(1, n, reply, 0)
    answer(me, zbox_ref)

    def settle(i, carry):
        arrival(i, ans, zbox_ref, send_back, recv_back).wait_recv()
        copy(i, ans, zbox_ref, send_back, recv_back).wait_send()
        copy(i, box_ref, inbox, send, recv).wait_send()
        if first:
            tags_to(i).wait_send()
        return carry

    lax.fori_loop(1, n, settle, 0)


def on_device(
    tile_data, tile_row, tile_col, tile_count, touched, owner_map, observed, start_x, start_u
):
    shards = lax.axis_size(AXES)
    local_cols = touched.shape[1]
    col_blocks = owner_map.shape[0]
    col_dev = col_blocks // shards
    capacity = max(1, (local_cols + shards - 1) // shards)
    row_blocks = observed.shape[0]
    slots, blk, _ = tile_data.shape
    targets = start_x.shape[2]
    boxes = shards * capacity
    f32, b16 = jnp.float32, jnp.bfloat16
    shape = jax.ShapeDtypeStruct

    wanted = touched[0]
    matches = (wanted[:, None] == jnp.arange(col_blocks, dtype=jnp.int32)[None, :]).astype(
        jnp.int32
    )
    position = jnp.sum(matches * owner_map[None, :], axis=1)
    owner = position // col_dev
    local_slot = position - owner * col_dev
    slot_order = jnp.arange(local_cols, dtype=jnp.int32)
    earlier = (owner[:, None] == owner[None, :]) & (slot_order[:, None] > slot_order[None, :])
    mailbox = owner * capacity + jnp.sum(earlier.astype(jnp.int32), axis=1)
    hit = mailbox[:, None] == jnp.arange(boxes, dtype=jnp.int32)[None, :]
    tags = jnp.sum(jnp.where(hit, local_slot[:, None] + 1, 0), axis=0) - 1
    tag_rows = -(-capacity // 8) * 8
    tags = jnp.pad(
        tags.astype(f32).reshape(shards, capacity),
        ((0, 0), (0, tag_rows - capacity)),
        constant_values=-1.0,
    )
    tags = jnp.broadcast_to(tags[:, :, None], (shards, tag_rows, blk))
    mailbox = mailbox[None, :]

    x = jnp.swapaxes(start_x, 1, 2)
    u = jnp.swapaxes(start_u, 1, 2)
    obs = jnp.swapaxes(observed, 1, 2)
    vec = (local_cols, targets, blk)
    big = 40 * MIB

    fwd, bwd, base, box = pl.pallas_call(
        prepare_kernel,
        out_shape=(
            shape((slots, 2 * blk, blk), b16),
            shape((slots, 2 * blk, blk), b16),
            shape(vec, f32),
            shape((boxes, targets, blk), f32),
        ),
        in_specs=[smem()] * 4 + [vmem()] * 4,
        out_specs=(vmem(),) * 4,
        scratch_shapes=[
            pltpu.VMEM((local_cols, 2 * targets, blk), b16),
            pltpu.VMEM((row_blocks, targets, blk), f32),
            pltpu.VMEM((row_blocks, 2 * targets, blk), b16),
        ],
        compiler_params=pltpu.CompilerParams(vmem_limit_bytes=big),
        name="prepare",
    )(tile_row, tile_col, tile_count, mailbox, tile_data, obs, x, u)

    def agree(first, box, tags):
        outs = [shape((boxes, targets, blk), f32), shape((col_dev, targets, blk), f32)]
        sems = [pltpu.SemaphoreType.DMA((shards,))] * 4
        if first:
            outs.append(shape(tags.shape, f32))
            sems = sems + [pltpu.SemaphoreType.DMA((shards,))] * 2
        return pl.pallas_call(
            functools.partial(agree_kernel, first, shards, capacity, col_dev),
            out_shape=tuple(outs),
            in_specs=[vmem()] * 2,
            out_specs=(vmem(),) * len(outs),
            scratch_shapes=[
                pltpu.VMEM((boxes, targets, blk), f32),
                pltpu.VMEM((boxes, targets, blk), f32),
            ] + sems,
            compiler_params=pltpu.CompilerParams(
                vmem_limit_bytes=big, has_side_effects=True
            ),
            name="agree",
        )(box, tags)

    for outer_step in range(ITERS):
        first, last = outer_step == 0, outer_step == ITERS - 1
        if first:
            zbox, zown, tags = agree(True, box, tags)
        else:
            zbox, zown = agree(False, box, tags)
        common = [
            pltpu.VMEM(vec, f32),
            pltpu.VMEM(vec, f32),
            pltpu.VMEM((local_cols, 2 * targets, blk), b16),
            pltpu.VMEM((row_blocks, targets, blk), f32),
            pltpu.VMEM((row_blocks, 2 * targets, blk), b16),
        ]
        if last:
            outs = (shape(vec, f32), shape(vec, f32), shape((targets, blk), f32))
            common = [pltpu.VMEM(vec, f32)] + common
        else:
            outs = (
                shape(vec, f32), shape(vec, f32), shape((boxes, targets, blk), f32),
                shape(vec, f32),
            )
        result = pl.pallas_call(
            functools.partial(solve_kernel, last),
            out_shape=outs,
            in_specs=[smem()] * 4 + [vmem()] * 6,
            out_specs=(vmem(),) * len(outs),
            scratch_shapes=common,
            compiler_params=pltpu.CompilerParams(vmem_limit_bytes=big),
            name="solve",
        )(tile_row, tile_col, tile_count, mailbox, fwd, bwd, base, x, u, zbox)
        if last:
            x, u, gap = result
        else:
            x, u, box, base = result
    gap_total = lax.psum(jnp.sum(gap, axis=1), AXES)
    primal_gap = jnp.sqrt(gap_total / (shards * local_cols * blk))
    return (jnp.swapaxes(x, 1, 2), jnp.swapaxes(u, 1, 2), jnp.swapaxes(zown, 1, 2), primal_gap)


def solution(mesh):
    both = P(AXES)
    placed = (
        P(AXES, None, None), P(AXES, None), P(AXES, None), both, P(AXES, None), P(),
        P(AXES, None, None), P(AXES, None, None), P(AXES, None, None),
    )
    return jax.shard_map(
        on_device,
        mesh=mesh,
        in_specs=placed,
        out_specs=(P(AXES, None, None), P(AXES, None, None), P(AXES, None, None), P()),
        check_vma=False,
    )
```

```python
import functools
import math

import jax
import jax.numpy as jnp
from jax import lax
from jax.experimental import pallas as pl
from jax.experimental.pallas import tpu as pltpu
from jax.sharding import PartitionSpec as P

ITERS = 2
CG_STEPS = 4
PENALTY = 1.0
COUPLING = 1.0
AXES = ("dev", "ka")
MESH = pl.DeviceIdType.MESH
MIB = 1 << 20


def vmem():
    return pl.BlockSpec(memory_space=pltpu.VMEM)


def smem():
    return pl.BlockSpec(memory_space=pltpu.SMEM)


def split(value):
    high = value.astype(jnp.bfloat16)
    low = (value - high.astype(jnp.float32)).astype(jnp.bfloat16)
    return jnp.concatenate([high, low], axis=0)


def tile_pass(tiles_ref, from_ids, to_ids, in_count, source_ref, target_ref):
    group = math.gcd(16, tiles_ref.shape[0])
    half = source_ref.shape[1] // 2

    def add_group(number, carry):
        for inner in range(group):
            t = number * group + inner
            lhs = source_ref[from_ids[0, t]]
            out = jnp.dot(
                jnp.concatenate([lhs, lhs], axis=1),
                tiles_ref[t],
                preferred_element_type=jnp.float32,
            )
            landing = to_ids[0, t]
            target_ref[landing] = target_ref[landing] + (out[:half] + out[half:])
        return carry

    lax.fori_loop(0, (in_count + group - 1) // group, add_group, 0)


def fill_zero(ref):
    def one(i, carry):
        ref[i] = jnp.zeros(ref.shape[1:], ref.dtype)
        return carry

    lax.fori_loop(0, ref.shape[0], one, 0, unroll=4)


def lanes(total):
    return jnp.sum(total, axis=1, keepdims=True)


def prepare_kernel(
    rows, cols, count, mailbox, tile_ref, obs_ref, x_ref, u_ref,
    fwd_ref, bwd_ref, base_ref, box_ref, xb_ref, w_ref, wb_ref,
):
    in_count = count[0]
    slots = tile_ref.shape[0]
    local_cols, targets, blk = x_ref.shape

    if box_ref.shape[0] != local_cols:
        fill_zero(box_ref)

    def convert(t, carry):
        tile = jnp.where(t < in_count, tile_ref[t], 0.0)
        bwd_ref[t] = split(tile)
        fwd_ref[t] = split(tile.T)
        return carry

    lax.fori_loop(0, slots, convert, 0, unroll=4)

    def begin(c, carry):
        x = x_ref[c]
        box_ref[mailbox[0, c]] = x + u_ref[c]
        xb_ref[c] = split(x)
        base_ref[c] = -x * COUPLING
        return carry

    lax.fori_loop(0, local_cols, begin, 0, unroll=4)
    fill_zero(w_ref)
    tile_pass(fwd_ref, cols, rows, in_count, xb_ref, w_ref)

    def against(r, carry):
        wb_ref[r] = split(obs_ref[r] - w_ref[r])
        return carry

    lax.fori_loop(0, w_ref.shape[0], against, 0, unroll=4)
    tile_pass(bwd_ref, rows, cols, in_count, wb_ref, base_ref)


def solve_kernel(
    last, rows, cols, count, mailbox, fwd_ref, bwd_ref, base_ref, x_ref, u_ref, zbox_ref,
    newx_ref, newu_ref, *rest,
):
    if last:
        r_ref, p_ref, q_ref, pb_ref, w_ref, wb_ref = rest
    else:
        box_ref, r_ref, p_ref, q_ref, pb_ref, w_ref, wb_ref = rest
    in_count = count[0]
    local_cols, targets, blk = x_ref.shape
    row_blocks = w_ref.shape[0]
    zero = jnp.zeros((targets, blk), jnp.float32)

    def begin(c, rr):
        z = zbox_ref[mailbox[0, c]]
        d = x_ref[c] - z
        u = u_ref[c] + d
        newu_ref[c] = u
        newx_ref[c] = x_ref[c]
        r = base_ref[c] + COUPLING * (z - u)
        r_ref[c] = r
        p_ref[c] = r
        q_ref[c] = COUPLING * r
        pb_ref[c] = split(r)
        return rr + r * r

    rr = lanes(lax.fori_loop(0, local_cols, begin, zero, unroll=2))
    pp = rr
    for step in range(CG_STEPS):
        final = last and step == CG_STEPS - 1
        fill_zero(w_ref)
        tile_pass(fwd_ref, cols, rows, in_count, pb_ref, w_ref)

        def image(i, ww):
            w = w_ref[i]
            if not final:
                wb_ref[i] = split(w)
            return ww + w * w

        ww = lanes(lax.fori_loop(0, row_blocks, image, zero, unroll=4))
        size = rr / (ww + COUPLING * pp)
        if final:

            def finish(c, carry):
                newx_ref[c] = newx_ref[c] + size * p_ref[c]
                return carry

            lax.fori_loop(0, local_cols, finish, 0, unroll=4)
            break
        tile_pass(bwd_ref, rows, cols, in_count, wb_ref, q_ref)

        def reduce(c, total):
            r = r_ref[c] - size * q_ref[c]
            r_ref[c] = r
            return total + r * r

        if step == CG_STEPS - 1:

            def close(c, carry):
                x = newx_ref[c] + size * p_ref[c]
                newx_ref[c] = x
                r = r_ref[c] - size * q_ref[c]
                slot = mailbox[0, c]
                u = newu_ref[c]
                box_ref[slot] = x + u
                base_ref_out[c] = r - COUPLING * (zbox_ref[slot] - u)
                return carry

            base_ref_out = r_ref
            if box_ref.shape[0] != local_cols:
                fill_zero(box_ref)
            lax.fori_loop(0, local_cols, close, 0, unroll=2)
            break
        norm = lanes(lax.fori_loop(0, local_cols, reduce, zero, unroll=4))
        turn = norm / rr

        def direct(c, total):
            old = p_ref[c]
            newx_ref[c] = newx_ref[c] + size * old
            p = r_ref[c] + turn * old
            p_ref[c] = p
            q_ref[c] = COUPLING * p
            pb_ref[c] = split(p)
            return total + p * p

        pp = lanes(lax.fori_loop(0, local_cols, direct, zero, unroll=2))
        rr = norm


def agree_kernel(first, last, capacity, col_dev, mean_of, *refs):
    refs = list(refs)
    box_ref, tag_ref = refs.pop(0), refs.pop(0)
    if not first:
        share_ref = refs.pop(0)
    if last:
        mailbox, x_ref = refs.pop(0), refs.pop(0)
    zbox_ref, zown_ref = refs.pop(0), refs.pop(0)
    if first:
        got_ref, share_ref = refs.pop(0), refs.pop(0)
    else:
        got_ref = tag_ref
    if last:
        gap_ref = refs.pop(0)
    inbox, ans, part_ref, far_ref, zall_ref = refs[:5]
    send, recv, back_send, back_recv, far_send, far_recv, all_send, all_recv = refs[5:13]
    refs = refs[13:]
    if first:
        count_ref, far_count, tag_send, tag_recv, count_send, count_recv = refs
    if last:
        gaps, gap_send, gap_recv = refs

    nd, nk = lax.axis_size(AXES[0]), lax.axis_size(AXES[1])
    n = nd * nk
    md, mk = lax.axis_index(AXES[0]), lax.axis_index(AXES[1])

    def after(i):
        return lax.rem(md + i, nd)

    def before(i):
        return lax.rem(md + nd - i, nd)

    def remote(source, target, send_sem, recv_sem, device):
        return pltpu.make_async_remote_copy(
            source, target, send_sem, recv_sem, device_id=device, device_id_type=MESH
        )

    def cell(d, k):
        return pl.ds((d * nk + k) * capacity, capacity)

    def tags_of(d):
        return pl.ds(d * nk, nk)

    def tags_to(i):
        return remote(
            tag_ref.at[tags_of(after(i))], got_ref.at[tags_of(md)],
            tag_send.at[i], tag_recv.at[i], (after(i), mk),
        )

    def tags_from(i):
        return remote(
            tag_ref.at[tags_of(before(i))], got_ref.at[tags_of(before(i))],
            tag_send.at[i], tag_recv.at[i], (before(i), mk),
        )

    def plane_to(i, k, source, target, sems):
        return remote(
            source.at[cell(after(i), k)], target.at[cell(md, k)],
            sems[0].at[i, k], sems[1].at[i, k], (after(i), mk),
        )

    def plane_from(i, k, source, target, sems):
        return remote(
            source.at[cell(before(i), k)], target.at[cell(before(i), k)],
            sems[0].at[i, k], sems[1].at[i, k], (before(i), mk),
        )

    there, back = (send, recv), (back_send, back_recv)

    def blocks(k):
        return pl.ds(k * col_dev, col_dev)

    def to_owner(o):
        k = lax.rem(mk + o, nk)
        return remote(
            part_ref.at[blocks(k)], far_ref.at[blocks(o)], far_send.at[o], far_recv.at[o],
            (md, k),
        )

    def count_to_owner(o):
        k = lax.rem(mk + o, nk)
        return remote(
            count_ref.at[k], far_count.at[o], count_send.at[o], count_recv.at[o], (md, k)
        )

    def from_owner(o):
        k = lax.rem(mk + o, nk)
        return remote(
            zown_ref, zall_ref.at[blocks(nk - o)], all_send.at[o], all_recv.at[o], (md, k)
        )

    order = list(range(1, nk)) + [0]
    if first:

        def start_tags(i, carry):
            tags_to(i).start()
            return carry

        lax.fori_loop(1, nd, start_tags, 0)
    for o in order:
        k = lax.rem(mk + o, nk)

        def start(i, carry):
            plane_to(i, k, box_ref, inbox, there).start()
            return carry

        lax.fori_loop(1, nd, start, 0)
    if first:
        got_ref[tags_of(md)] = tag_ref[tags_of(md)]
        count_ref[...] = jnp.zeros_like(count_ref)
    part_ref[...] = jnp.zeros_like(part_ref)

    def take(source_ref, d, k):
        for j in range(capacity):
            value = source_ref[(d * nk + k) * capacity + j]
            tag = got_ref[d * nk + k, pl.ds(j, 1)]
            for b in range(col_dev):
                at = k * col_dev + b
                part_ref[at] = part_ref[at] + jnp.where(tag == b, value, 0.0)
                if first:
                    spot = pl.ds(b, 1)
                    count_ref[k, spot] = count_ref[k, spot] + jnp.where(tag == b, 1.0, 0.0)

    for position, o in enumerate(order):
        k = lax.rem(mk + o, nk)
        take(box_ref, md, k)

        def collect(i, carry):
            if first and position == 0:
                tags_from(i).wait_recv()
            plane_from(i, k, box_ref, inbox, there).wait_recv()
            take(inbox, before(i), k)
            return carry

        lax.fori_loop(1, nd, collect, 0)
        if o:
            to_owner(o).start()
            if first:
                count_to_owner(o).start()

    for b in range(col_dev):
        zown_ref[b] = part_ref[mk * col_dev + b]
    if first:
        share_ref[...] = count_ref[mk]
    for o in range(1, nk):
        to_owner(o).wait_recv()
        for b in range(col_dev):
            zown_ref[b] = zown_ref[b] + far_ref[o * col_dev + b]
        if first:
            count_to_owner(o).wait_recv()
            share_ref[...] = share_ref[...] + far_count[o]
    for b in range(col_dev):
        share = jnp.maximum(share_ref[pl.ds(b, 1)], 1.0)
        amount = zown_ref[b] / share
        cutoff = PENALTY / (COUPLING * share)
        z = amount - jnp.clip(amount, -cutoff, cutoff)
        zown_ref[b] = z
        zall_ref[b] = z
    for o in range(1, nk):
        from_owner(o).start()

    def answer(d, k, slot, target_ref):
        for j in range(capacity):
            tag = got_ref[d * nk + k, pl.ds(j, 1)]
            value = jnp.where(tag == 0, zall_ref[slot * col_dev], 0.0)
            for b in range(1, col_dev):
                value = value + jnp.where(tag == b, zall_ref[slot * col_dev + b], 0.0)
            target_ref[(d * nk + k) * capacity + j] = value

    for o in range(nk):
        k = lax.rem(mk + o, nk)
        if o:
            from_owner(nk - o).wait_recv()

        def reply(i, carry):
            answer(after(i), k, o, ans)
            plane_to(i, k, ans, zbox_ref, back).start()
            return carry

        lax.fori_loop(1, nd, reply, 0)
        answer(md, k, o, zbox_ref)

    for o in range(nk):
        k = lax.rem(mk + o, nk)

        def settle(i, carry):
            plane_from(i, k, ans, zbox_ref, back).wait_recv()
            return carry

        lax.fori_loop(1, nd, settle, 0)

    if last:
        me = md * nk + mk

        def gap_to(i):
            device = lax.rem(me + i, n)
            return remote(
                gaps.at[me], gaps.at[me], gap_send.at[i], gap_recv.at[i],
                (device // nk, lax.rem(device, nk)),
            )

        def gap_from(i):
            device = lax.rem(me + n - i, n)
            return remote(
                gaps.at[device], gaps.at[device], gap_send.at[i], gap_recv.at[i],
                (device // nk, lax.rem(device, nk)),
            )

        targets, blk = x_ref.shape[1:]

        def square(c, total):
            d = x_ref[c] - zbox_ref[mailbox[0, c]]
            return total + d * d

        zero = jnp.zeros((targets, blk), jnp.float32)
        total = lax.fori_loop(0, x_ref.shape[0], square, zero)
        width = gaps.shape[2]
        if width > targets:
            total = jnp.concatenate(
                [total, jnp.zeros((width - targets, blk), jnp.float32)], axis=0
            )
        gaps[me] = lax.dot_general(
            jnp.ones((8, blk), jnp.float32), total, (((1,), (1,)), ((), ())),
            precision=lax.Precision.HIGHEST, preferred_element_type=jnp.float32,
        )

        def tell(i, carry):
            gap_to(i).start()
            return carry

        lax.fori_loop(1, n, tell, 0)

        def heard(i, carry):
            gap_from(i).wait_recv()
            return carry

        lax.fori_loop(1, n, heard, 0)
        whole = lax.fori_loop(
            0, n, lambda i, t: t + gaps[i], jnp.zeros((8, width), jnp.float32)
        )
        gap_ref[...] = jnp.sqrt(whole / mean_of)

        def told(i, carry):
            gap_to(i).wait_send()
            return carry

        lax.fori_loop(1, n, told, 0)

    for o in range(nk):
        k = lax.rem(mk + o, nk)

        def sent(i, carry):
            plane_to(i, k, box_ref, inbox, there).wait_send()
            plane_to(i, k, ans, zbox_ref, back).wait_send()
            if first and o == 0:
                tags_to(i).wait_send()
            return carry

        lax.fori_loop(1, nd, sent, 0)
        if o:
            to_owner(o).wait_send()
            from_owner(o).wait_send()
            if first:
                count_to_owner(o).wait_send()


def on_device(
    tile_data, tile_row, tile_col, tile_count, touched, owner_map, observed, start_x, start_u
):
    shards = lax.axis_size(AXES)
    local_cols = touched.shape[1]
    col_blocks = owner_map.shape[0]
    col_dev = col_blocks // shards
    capacity = max(1, (local_cols + shards - 1) // shards)
    row_blocks = observed.shape[0]
    slots, blk, _ = tile_data.shape
    targets = start_x.shape[2]
    boxes = shards * capacity
    f32, b16 = jnp.float32, jnp.bfloat16
    shape = jax.ShapeDtypeStruct

    wanted = touched[0]
    matches = (wanted[:, None] == jnp.arange(col_blocks, dtype=jnp.int32)[None, :]).astype(
        jnp.int32
    )
    position = jnp.sum(matches * owner_map[None, :], axis=1)
    owner = position // col_dev
    local_slot = position - owner * col_dev
    slot_order = jnp.arange(local_cols, dtype=jnp.int32)
    earlier = (owner[:, None] == owner[None, :]) & (slot_order[:, None] > slot_order[None, :])
    mailbox = owner * capacity + jnp.sum(earlier.astype(jnp.int32), axis=1)
    hit = mailbox[:, None] == jnp.arange(boxes, dtype=jnp.int32)[None, :]
    tags = jnp.sum(jnp.where(hit, local_slot[:, None] + 1, 0), axis=0) - 1
    tag_rows = -(-capacity // 8) * 8
    tags = jnp.pad(
        tags.astype(f32).reshape(shards, capacity),
        ((0, 0), (0, tag_rows - capacity)),
        constant_values=-1.0,
    )
    tags = jnp.broadcast_to(tags[:, :, None], (shards, tag_rows, blk))
    mailbox = mailbox[None, :]

    x = jnp.swapaxes(start_x, 1, 2)
    u = jnp.swapaxes(start_u, 1, 2)
    obs = jnp.swapaxes(observed, 1, 2)
    vec = (local_cols, targets, blk)
    big = 40 * MIB

    fwd, bwd, base, box = pl.pallas_call(
        prepare_kernel,
        out_shape=(
            shape((slots, 2 * blk, blk), b16),
            shape((slots, 2 * blk, blk), b16),
            shape(vec, f32),
            shape((boxes, targets, blk), f32),
        ),
        in_specs=[smem()] * 4 + [vmem()] * 4,
        out_specs=(vmem(),) * 4,
        scratch_shapes=[
            pltpu.VMEM((local_cols, 2 * targets, blk), b16),
            pltpu.VMEM((row_blocks, targets, blk), f32),
            pltpu.VMEM((row_blocks, 2 * targets, blk), b16),
        ],
        compiler_params=pltpu.CompilerParams(vmem_limit_bytes=big),
        name="prepare",
    )(tile_row, tile_col, tile_count, mailbox, tile_data, obs, x, u)

    nd, nk = lax.axis_size(AXES[0]), lax.axis_size(AXES[1])
    count_rows = -(-col_dev // 8) * 8
    width = -(-targets // blk) * blk
    dma = pltpu.SemaphoreType.DMA

    def agree(first, last, *operands):
        outs = [shape((boxes, targets, blk), f32), shape((col_dev, targets, blk), f32)]
        specs = [vmem()] * len(operands)
        dense = pltpu.VMEM((nk * col_dev, targets, blk), f32)
        scratch = [
            pltpu.VMEM((boxes, targets, blk), f32),
            pltpu.VMEM((boxes, targets, blk), f32),
            dense, dense, dense,
        ] + [dma((nd, nk))] * 4 + [dma((nk,))] * 4
        if first:
            outs += [shape(tags.shape, f32), shape((count_rows, blk), f32)]
            counts = pltpu.VMEM((nk, count_rows, blk), f32)
            scratch += [counts, counts, dma((nd,)), dma((nd,)), dma((nk,)), dma((nk,))]
        if last:
            specs[-2] = smem()
            outs.append(shape((8, width), f32))
            scratch += [pltpu.VMEM((shards, 8, width), f32), dma((shards,)), dma((shards,))]
        mean_of = shards * local_cols * blk
        return pl.pallas_call(
            functools.partial(agree_kernel, first, last, capacity, col_dev, mean_of),
            out_shape=tuple(outs),
            in_specs=specs,
            out_specs=(vmem(),) * len(outs),
            scratch_shapes=scratch,
            compiler_params=pltpu.CompilerParams(
                vmem_limit_bytes=big, has_side_effects=True
            ),
            name="agree",
        )(*operands)

    for outer_step in range(ITERS):
        first, last = outer_step == 0, outer_step == ITERS - 1
        operands = [box, tags]
        if not first:
            operands.append(share)
        if last:
            operands += [mailbox, x]
        result = list(agree(first, last, *operands))
        zbox, zown = result[:2]
        if first:
            tags, share = result[2:4]
        if last:
            gap = result[-1]
        common = [
            pltpu.VMEM(vec, f32),
            pltpu.VMEM(vec, f32),
            pltpu.VMEM((local_cols, 2 * targets, blk), b16),
            pltpu.VMEM((row_blocks, targets, blk), f32),
            pltpu.VMEM((row_blocks, 2 * targets, blk), b16),
        ]
        if last:
            outs = (shape(vec, f32), shape(vec, f32))
            common = [pltpu.VMEM(vec, f32)] + common
        else:
            outs = (
                shape(vec, f32), shape(vec, f32), shape((boxes, targets, blk), f32),
                shape(vec, f32),
            )
        result = pl.pallas_call(
            functools.partial(solve_kernel, last),
            out_shape=outs,
            in_specs=[smem()] * 4 + [vmem()] * 6,
            out_specs=(vmem(),) * len(outs),
            scratch_shapes=common,
            compiler_params=pltpu.CompilerParams(vmem_limit_bytes=big),
            name="solve",
        )(tile_row, tile_col, tile_count, mailbox, fwd, bwd, base, x, u, zbox)
        if last:
            x, u = result
        else:
            x, u, box, base = result
    primal_gap = gap[0, :targets]
    return (jnp.swapaxes(x, 1, 2), jnp.swapaxes(u, 1, 2), jnp.swapaxes(zown, 1, 2), primal_gap)


def solution(mesh):
    both = P(AXES)
    placed = (
        P(AXES, None, None), P(AXES, None), P(AXES, None), both, P(AXES, None), P(),
        P(AXES, None, None), P(AXES, None, None), P(AXES, None, None),
    )
    return jax.shard_map(
        on_device,
        mesh=mesh,
        in_specs=placed,
        out_specs=(P(AXES, None, None), P(AXES, None, None), P(AXES, None, None), P()),
        check_vma=False,
    )
```

```python
import functools
import math

import jax
import jax.numpy as jnp
from jax import lax
from jax.experimental import pallas as pl
from jax.experimental.pallas import tpu as pltpu
from jax.sharding import PartitionSpec as P

ITERS = 2
CG_STEPS = 4
PENALTY = 1.0
COUPLING = 1.0
AXES = ("dev", "ka")
MESH = pl.DeviceIdType.MESH
MIB = 1 << 20
PREP, AGREE, SOLVE = 26, 24, 24


def vmem():
    return pl.BlockSpec(memory_space=pltpu.VMEM)


def smem():
    return pl.BlockSpec(memory_space=pltpu.SMEM)


def split(value):
    high = value.astype(jnp.bfloat16)
    low = (value - high.astype(jnp.float32)).astype(jnp.bfloat16)
    return jnp.concatenate([high, low], axis=0)


def tile_pass(tiles_ref, from_ids, to_ids, in_count, source_ref, target_ref):
    group = math.gcd(16, tiles_ref.shape[0])
    half = source_ref.shape[1] // 2

    def add_group(number, carry):
        for inner in range(group):
            t = number * group + inner
            lhs = source_ref[from_ids[0, t]]
            out = jnp.dot(
                jnp.concatenate([lhs, lhs], axis=1),
                tiles_ref[t],
                preferred_element_type=jnp.float32,
            )
            landing = to_ids[0, t]
            target_ref[landing] = target_ref[landing] + (out[:half] + out[half:])
        return carry

    lax.fori_loop(0, (in_count + group - 1) // group, add_group, 0)


def fill_zero(ref):
    def one(i, carry):
        ref[i] = jnp.zeros(ref.shape[1:], ref.dtype)
        return carry

    lax.fori_loop(0, ref.shape[0], one, 0, unroll=4)


def lanes(total):
    return jnp.sum(total, axis=1, keepdims=True)


def prepare_kernel(
    rows, cols, count, mailbox, tile_hbm, obs_hbm, x_hbm, u_hbm,
    fwd_ref, bwd_ref, base_ref, box_ref,
    xb_ref, w_ref, wb_ref, tile_ref, obs_ref, x_ref, u_ref, sems,
):
    in_count = count[0]
    slots = tile_ref.shape[0]
    local_cols, targets, blk = x_ref.shape
    chunks = math.gcd(4, slots)
    chunk = slots // chunks
    half = math.gcd(2, local_cols)
    portion = local_cols // half

    def load(source, target, first, size, number):
        at = pl.ds(first, size)
        return pltpu.make_async_copy(source.at[at], target.at[at], sems.at[number])

    vectors = [
        (
            load(x_hbm, x_ref, i * portion, portion, 2 * i),
            load(u_hbm, u_ref, i * portion, portion, 2 * i + 1),
        )
        for i in range(half)
    ]
    tiles = [load(tile_hbm, tile_ref, i * chunk, chunk, 4 + i) for i in range(chunks)]
    responses = pltpu.make_async_copy(obs_hbm, obs_ref, sems.at[8])
    for pair in vectors:
        for one in pair:
            one.start()
    for one in tiles:
        one.start()
    responses.start()

    if box_ref.shape[0] != local_cols:
        fill_zero(box_ref)
    fill_zero(w_ref)

    def begin(c, carry):
        x = x_ref[c]
        box_ref[mailbox[0, c]] = x + u_ref[c]
        xb_ref[c] = split(x)
        base_ref[c] = -x * COUPLING
        return carry

    for i, pair in enumerate(vectors):
        for one in pair:
            one.wait()
        lax.fori_loop(i * portion, (i + 1) * portion, begin, 0, unroll=4)

    def convert(t, carry):
        tile = jnp.where(t < in_count, tile_ref[t], 0.0)
        bwd_ref[t] = split(tile)
        fwd_ref[t] = split(tile.T)
        return carry

    for i, one in enumerate(tiles):
        one.wait()
        lax.fori_loop(i * chunk, (i + 1) * chunk, convert, 0, unroll=4)

    tile_pass(fwd_ref, cols, rows, in_count, xb_ref, w_ref)
    responses.wait()

    def against(r, carry):
        wb_ref[r] = split(obs_ref[r] - w_ref[r])
        return carry

    lax.fori_loop(0, w_ref.shape[0], against, 0, unroll=4)
    tile_pass(bwd_ref, rows, cols, in_count, wb_ref, base_ref)


def solve_kernel(
    last, rows, cols, count, mailbox, fwd_ref, bwd_ref, base_ref, x_ref, u_ref, zbox_ref,
    newx_ref, newu_ref, *rest,
):
    if last:
        r_ref, p_ref, q_ref, pb_ref, w_ref, wb_ref = rest
    else:
        box_ref, r_ref, p_ref, q_ref, pb_ref, w_ref, wb_ref = rest
    in_count = count[0]
    local_cols, targets, blk = x_ref.shape
    row_blocks = w_ref.shape[0]
    zero = jnp.zeros((targets, blk), jnp.float32)

    def begin(c, rr):
        z = zbox_ref[mailbox[0, c]]
        d = x_ref[c] - z
        u = u_ref[c] + d
        newu_ref[c] = u
        r = base_ref[c] + COUPLING * (z - u)
        r_ref[c] = r
        p_ref[c] = r
        q_ref[c] = COUPLING * r
        pb_ref[c] = split(r)
        return rr + r * r

    rr = lanes(lax.fori_loop(0, local_cols, begin, zero, unroll=2))
    pp = rr
    for step in range(CG_STEPS):
        final = last and step == CG_STEPS - 1
        held_ref = x_ref if step == 0 else newx_ref
        fill_zero(w_ref)
        tile_pass(fwd_ref, cols, rows, in_count, pb_ref, w_ref)

        def image(i, ww):
            w = w_ref[i]
            if not final:
                wb_ref[i] = split(w)
            return ww + w * w

        ww = lanes(lax.fori_loop(0, row_blocks, image, zero, unroll=4))
        size = rr / (ww + COUPLING * pp)
        if final:

            def finish(c, carry):
                newx_ref[c] = held_ref[c] + size * p_ref[c]
                return carry

            lax.fori_loop(0, local_cols, finish, 0, unroll=4)
            break
        tile_pass(bwd_ref, rows, cols, in_count, wb_ref, q_ref)

        def reduce(c, total):
            r = r_ref[c] - size * q_ref[c]
            r_ref[c] = r
            return total + r * r

        if step == CG_STEPS - 1:

            def close(c, carry):
                x = held_ref[c] + size * p_ref[c]
                newx_ref[c] = x
                r = r_ref[c] - size * q_ref[c]
                slot = mailbox[0, c]
                u = newu_ref[c]
                box_ref[slot] = x + u
                base_ref_out[c] = r - COUPLING * (zbox_ref[slot] - u)
                return carry

            base_ref_out = r_ref
            if box_ref.shape[0] != local_cols:
                fill_zero(box_ref)
            lax.fori_loop(0, local_cols, close, 0, unroll=2)
            break
        norm = lanes(lax.fori_loop(0, local_cols, reduce, zero, unroll=4))
        turn = norm / rr

        def direct(c, total):
            old = p_ref[c]
            newx_ref[c] = held_ref[c] + size * old
            p = r_ref[c] + turn * old
            p_ref[c] = p
            q_ref[c] = COUPLING * p
            pb_ref[c] = split(p)
            return total + p * p

        pp = lanes(lax.fori_loop(0, local_cols, direct, zero, unroll=2))
        rr = norm


def agree_kernel(first, last, capacity, col_dev, mean_of, *refs):
    refs = list(refs)
    box_ref, tag_ref = refs.pop(0), refs.pop(0)
    if not first:
        share_ref = refs.pop(0)
    if last:
        mailbox, x_ref = refs.pop(0), refs.pop(0)
    zbox_ref, zown_ref = refs.pop(0), refs.pop(0)
    if first:
        got_ref, share_ref = refs.pop(0), refs.pop(0)
    else:
        got_ref = tag_ref
    if last:
        gap_ref = refs.pop(0)
    inbox, ans, part_ref, far_ref, zall_ref = refs[:5]
    send, recv, back_send, back_recv, far_send, far_recv, all_send, all_recv = refs[5:13]
    refs = refs[13:]
    if first:
        count_ref, far_count, tag_send, tag_recv, count_send, count_recv = refs
    if last:
        gaps, gap_send, gap_recv = refs

    nd, nk = lax.axis_size(AXES[0]), lax.axis_size(AXES[1])
    n = nd * nk
    md, mk = lax.axis_index(AXES[0]), lax.axis_index(AXES[1])

    def after(i):
        return lax.rem(md + i, nd)

    def before(i):
        return lax.rem(md + nd - i, nd)

    def remote(source, target, send_sem, recv_sem, device):
        return pltpu.make_async_remote_copy(
            source, target, send_sem, recv_sem, device_id=device, device_id_type=MESH
        )

    def cell(d, k):
        return pl.ds((d * nk + k) * capacity, capacity)

    def tags_of(d):
        return pl.ds(d * nk, nk)

    def tags_to(i):
        return remote(
            tag_ref.at[tags_of(after(i))], got_ref.at[tags_of(md)],
            tag_send.at[i], tag_recv.at[i], (after(i), mk),
        )

    def tags_from(i):
        return remote(
            tag_ref.at[tags_of(before(i))], got_ref.at[tags_of(before(i))],
            tag_send.at[i], tag_recv.at[i], (before(i), mk),
        )

    def plane_to(i, k, source, target, sems):
        return remote(
            source.at[cell(after(i), k)], target.at[cell(md, k)],
            sems[0].at[i, k], sems[1].at[i, k], (after(i), mk),
        )

    def plane_from(i, k, source, target, sems):
        return remote(
            source.at[cell(before(i), k)], target.at[cell(before(i), k)],
            sems[0].at[i, k], sems[1].at[i, k], (before(i), mk),
        )

    there, back = (send, recv), (back_send, back_recv)

    def blocks(k):
        return pl.ds(k * col_dev, col_dev)

    def to_owner(o):
        k = lax.rem(mk + o, nk)
        return remote(
            part_ref.at[blocks(k)], far_ref.at[blocks(o)], far_send.at[o], far_recv.at[o],
            (md, k),
        )

    def count_to_owner(o):
        k = lax.rem(mk + o, nk)
        return remote(
            count_ref.at[k], far_count.at[o], count_send.at[o], count_recv.at[o], (md, k)
        )

    def from_owner(o):
        k = lax.rem(mk + o, nk)
        return remote(
            zown_ref, zall_ref.at[blocks(nk - o)], all_send.at[o], all_recv.at[o], (md, k)
        )

    order = list(range(1, nk)) + [0]
    if first:

        def start_tags(i, carry):
            tags_to(i).start()
            return carry

        lax.fori_loop(1, nd, start_tags, 0)
    for o in order:
        k = lax.rem(mk + o, nk)

        def start(i, carry):
            plane_to(i, k, box_ref, inbox, there).start()
            return carry

        lax.fori_loop(1, nd, start, 0)
    if first:
        got_ref[tags_of(md)] = tag_ref[tags_of(md)]
        count_ref[...] = jnp.zeros_like(count_ref)
    part_ref[...] = jnp.zeros_like(part_ref)

    def take(source_ref, d, k):
        for j in range(capacity):
            value = source_ref[(d * nk + k) * capacity + j]
            tag = got_ref[d * nk + k, pl.ds(j, 1)]
            for b in range(col_dev):
                at = k * col_dev + b
                part_ref[at] = part_ref[at] + jnp.where(tag == b, value, 0.0)
                if first:
                    spot = pl.ds(b, 1)
                    count_ref[k, spot] = count_ref[k, spot] + jnp.where(tag == b, 1.0, 0.0)

    for position, o in enumerate(order):
        k = lax.rem(mk + o, nk)
        take(box_ref, md, k)

        def collect(i, carry):
            if first and position == 0:
                tags_from(i).wait_recv()
            plane_from(i, k, box_ref, inbox, there).wait_recv()
            take(inbox, before(i), k)
            return carry

        lax.fori_loop(1, nd, collect, 0)
        if o:
            to_owner(o).start()
            if first:
                count_to_owner(o).start()

    for b in range(col_dev):
        zown_ref[b] = part_ref[mk * col_dev + b]
    if first:
        share_ref[...] = count_ref[mk]
    for o in range(1, nk):
        to_owner(o).wait_recv()
        for b in range(col_dev):
            zown_ref[b] = zown_ref[b] + far_ref[o * col_dev + b]
        if first:
            count_to_owner(o).wait_recv()
            share_ref[...] = share_ref[...] + far_count[o]
    for b in range(col_dev):
        share = jnp.maximum(share_ref[pl.ds(b, 1)], 1.0)
        amount = zown_ref[b] / share
        cutoff = PENALTY / (COUPLING * share)
        z = amount - jnp.clip(amount, -cutoff, cutoff)
        zown_ref[b] = z
        zall_ref[b] = z
    for o in range(1, nk):
        from_owner(o).start()

    def answer(d, k, slot, target_ref):
        for j in range(capacity):
            tag = got_ref[d * nk + k, pl.ds(j, 1)]
            value = jnp.where(tag == 0, zall_ref[slot * col_dev], 0.0)
            for b in range(1, col_dev):
                value = value + jnp.where(tag == b, zall_ref[slot * col_dev + b], 0.0)
            target_ref[(d * nk + k) * capacity + j] = value

    for o in range(nk):
        k = lax.rem(mk + o, nk)
        if o:
            from_owner(nk - o).wait_recv()

        def reply(i, carry):
            answer(after(i), k, o, ans)
            plane_to(i, k, ans, zbox_ref, back).start()
            return carry

        lax.fori_loop(1, nd, reply, 0)
        answer(md, k, o, zbox_ref)

    for o in range(nk):
        k = lax.rem(mk + o, nk)

        def settle(i, carry):
            plane_from(i, k, ans, zbox_ref, back).wait_recv()
            return carry

        lax.fori_loop(1, nd, settle, 0)

    if last:
        me = md * nk + mk

        def gap_to(i):
            device = lax.rem(me + i, n)
            return remote(
                gaps.at[me], gaps.at[me], gap_send.at[i], gap_recv.at[i],
                (device // nk, lax.rem(device, nk)),
            )

        def gap_from(i):
            device = lax.rem(me + n - i, n)
            return remote(
                gaps.at[device], gaps.at[device], gap_send.at[i], gap_recv.at[i],
                (device // nk, lax.rem(device, nk)),
            )

        targets, blk = x_ref.shape[1:]

        def square(c, total):
            d = x_ref[c] - zbox_ref[mailbox[0, c]]
            return total + d * d

        zero = jnp.zeros((targets, blk), jnp.float32)
        total = lax.fori_loop(0, x_ref.shape[0], square, zero)
        width = gaps.shape[2]
        if width > targets:
            total = jnp.concatenate(
                [total, jnp.zeros((width - targets, blk), jnp.float32)], axis=0
            )
        gaps[me] = lax.dot_general(
            jnp.ones((8, blk), jnp.float32), total, (((1,), (1,)), ((), ())),
            precision=lax.Precision.HIGHEST, preferred_element_type=jnp.float32,
        )

        def tell(i, carry):
            gap_to(i).start()
            return carry

        lax.fori_loop(1, n, tell, 0)

        def heard(i, carry):
            gap_from(i).wait_recv()
            return carry

        lax.fori_loop(1, n, heard, 0)
        whole = lax.fori_loop(
            0, n, lambda i, t: t + gaps[i], jnp.zeros((8, width), jnp.float32)
        )
        gap_ref[...] = jnp.sqrt(whole / mean_of)

        def told(i, carry):
            gap_to(i).wait_send()
            return carry

        lax.fori_loop(1, n, told, 0)

    for o in range(nk):
        k = lax.rem(mk + o, nk)

        def sent(i, carry):
            plane_to(i, k, box_ref, inbox, there).wait_send()
            plane_to(i, k, ans, zbox_ref, back).wait_send()
            if first and o == 0:
                tags_to(i).wait_send()
            return carry

        lax.fori_loop(1, nd, sent, 0)
        if o:
            to_owner(o).wait_send()
            from_owner(o).wait_send()
            if first:
                count_to_owner(o).wait_send()


def on_device(
    tile_data, tile_row, tile_col, tile_count, touched, owner_map, observed, start_x, start_u
):
    shards = lax.axis_size(AXES)
    local_cols = touched.shape[1]
    col_blocks = owner_map.shape[0]
    col_dev = col_blocks // shards
    capacity = max(1, (local_cols + shards - 1) // shards)
    row_blocks = observed.shape[0]
    slots, blk, _ = tile_data.shape
    targets = start_x.shape[2]
    boxes = shards * capacity
    f32, b16 = jnp.float32, jnp.bfloat16
    shape = jax.ShapeDtypeStruct

    wanted = touched[0]
    matches = (wanted[:, None] == jnp.arange(col_blocks, dtype=jnp.int32)[None, :]).astype(
        jnp.int32
    )
    position = jnp.sum(matches * owner_map[None, :], axis=1)
    owner = position // col_dev
    local_slot = position - owner * col_dev
    slot_order = jnp.arange(local_cols, dtype=jnp.int32)
    earlier = (owner[:, None] == owner[None, :]) & (slot_order[:, None] > slot_order[None, :])
    mailbox = owner * capacity + jnp.sum(earlier.astype(jnp.int32), axis=1)
    hit = mailbox[:, None] == jnp.arange(boxes, dtype=jnp.int32)[None, :]
    tags = jnp.sum(jnp.where(hit, local_slot[:, None] + 1, 0), axis=0) - 1
    tag_rows = -(-capacity // 8) * 8
    tags = jnp.pad(
        tags.astype(f32).reshape(shards, capacity),
        ((0, 0), (0, tag_rows - capacity)),
        constant_values=-1.0,
    )
    tags = jnp.broadcast_to(tags[:, :, None], (shards, tag_rows, blk))
    mailbox = mailbox[None, :]

    x = jnp.swapaxes(start_x, 1, 2)
    u = jnp.swapaxes(start_u, 1, 2)
    obs = jnp.swapaxes(observed, 1, 2)
    vec = (local_cols, targets, blk)

    fwd, bwd, base, box = pl.pallas_call(
        prepare_kernel,
        out_shape=(
            shape((slots, 2 * blk, blk), b16),
            shape((slots, 2 * blk, blk), b16),
            shape(vec, f32),
            shape((boxes, targets, blk), f32),
        ),
        in_specs=[smem()] * 4 + [pl.BlockSpec(memory_space=pltpu.HBM)] * 4,
        out_specs=(vmem(),) * 4,
        scratch_shapes=[
            pltpu.VMEM((local_cols, 2 * targets, blk), b16),
            pltpu.VMEM((row_blocks, targets, blk), f32),
            pltpu.VMEM((row_blocks, 2 * targets, blk), b16),
            pltpu.VMEM((slots, blk, blk), f32),
            pltpu.VMEM((row_blocks, targets, blk), f32),
            pltpu.VMEM(vec, f32),
            pltpu.VMEM(vec, f32),
            pltpu.SemaphoreType.DMA((9,)),
        ],
        compiler_params=pltpu.CompilerParams(vmem_limit_bytes=PREP * MIB),
        name="prepare",
    )(tile_row, tile_col, tile_count, mailbox, tile_data, obs, x, u)

    nd, nk = lax.axis_size(AXES[0]), lax.axis_size(AXES[1])
    count_rows = -(-col_dev // 8) * 8
    width = -(-targets // blk) * blk
    dma = pltpu.SemaphoreType.DMA

    def agree(first, last, *operands):
        outs = [shape((boxes, targets, blk), f32), shape((col_dev, targets, blk), f32)]
        specs = [vmem()] * len(operands)
        dense = pltpu.VMEM((nk * col_dev, targets, blk), f32)
        scratch = [
            pltpu.VMEM((boxes, targets, blk), f32),
            pltpu.VMEM((boxes, targets, blk), f32),
            dense, dense, dense,
        ] + [dma((nd, nk))] * 4 + [dma((nk,))] * 4
        if first:
            outs += [shape(tags.shape, f32), shape((count_rows, blk), f32)]
            counts = pltpu.VMEM((nk, count_rows, blk), f32)
            scratch += [counts, counts, dma((nd,)), dma((nd,)), dma((nk,)), dma((nk,))]
        if last:
            specs[-2] = smem()
            outs.append(shape((8, width), f32))
            scratch += [pltpu.VMEM((shards, 8, width), f32), dma((shards,)), dma((shards,))]
        mean_of = shards * local_cols * blk
        return pl.pallas_call(
            functools.partial(agree_kernel, first, last, capacity, col_dev, mean_of),
            out_shape=tuple(outs),
            in_specs=specs,
            out_specs=(vmem(),) * len(outs),
            scratch_shapes=scratch,
            compiler_params=pltpu.CompilerParams(
                vmem_limit_bytes=AGREE * MIB, has_side_effects=True
            ),
            name="agree",
        )(*operands)

    for outer_step in range(ITERS):
        first, last = outer_step == 0, outer_step == ITERS - 1
        operands = [box, tags]
        if not first:
            operands.append(share)
        if last:
            operands += [mailbox, x]
        result = list(agree(first, last, *operands))
        zbox, zown = result[:2]
        if first:
            tags, share = result[2:4]
        if last:
            gap = result[-1]
        common = [
            pltpu.VMEM(vec, f32),
            pltpu.VMEM(vec, f32),
            pltpu.VMEM((local_cols, 2 * targets, blk), b16),
            pltpu.VMEM((row_blocks, targets, blk), f32),
            pltpu.VMEM((row_blocks, 2 * targets, blk), b16),
        ]
        if last:
            outs = (shape(vec, f32), shape(vec, f32))
            common = [pltpu.VMEM(vec, f32)] + common
        else:
            outs = (
                shape(vec, f32), shape(vec, f32), shape((boxes, targets, blk), f32),
                shape(vec, f32),
            )
        result = pl.pallas_call(
            functools.partial(solve_kernel, last),
            out_shape=outs,
            in_specs=[smem()] * 4 + [vmem()] * 6,
            out_specs=(vmem(),) * len(outs),
            scratch_shapes=common,
            compiler_params=pltpu.CompilerParams(vmem_limit_bytes=SOLVE * MIB),
            name="solve",
        )(tile_row, tile_col, tile_count, mailbox, fwd, bwd, base, x, u, zbox)
        if last:
            x, u = result
        else:
            x, u, box, base = result
    primal_gap = gap[0, :targets]
    return (jnp.swapaxes(x, 1, 2), jnp.swapaxes(u, 1, 2), jnp.swapaxes(zown, 1, 2), primal_gap)


def solution(mesh):
    both = P(AXES)
    placed = (
        P(AXES, None, None), P(AXES, None), P(AXES, None), both, P(AXES, None), P(),
        P(AXES, None, None), P(AXES, None, None), P(AXES, None, None),
    )
    return jax.shard_map(
        on_device,
        mesh=mesh,
        in_specs=placed,
        out_specs=(P(AXES, None, None), P(AXES, None, None), P(AXES, None, None), P()),
        check_vma=False,
    )
```
